32 devices in a mesh: pairs: 8 (over z, x), stream: 4 (over y, core).
Axes of the slice: x: 2, y: 2, z: 4, core: 2. Of those that a mesh axis runs over, the one named last changes fastest.
Arguments:
- images: bfloat16 [48, 576, 768], P('pairs', 'stream'), may hold values from -6 to 6
- captions: bfloat16 [48, 40, 768], P('pairs', 'stream'), may hold values from -6 to 6
- lengths: int32 [48], P('pairs'), may hold values from 8 to 40
- first_gain: float32 [768], replicated, may hold values from 0.1 to 1.9
- first_shift: float32 [768], replicated, may hold values from -3 to 3
- query_key_value: bfloat16 [768, 2304], replicated, may hold values from -0.21875 to 0.21875
- query_bias: float32 [768], replicated, may hold values from -3 to 3
- value_bias: float32 [768], replicated, may hold values from -3 to 3
- output_weight: bfloat16 [768, 768], replicated, may hold values from -1.25 to 1.25
- output_bias: float32 [768], replicated, may hold values from -3 to 3
- second_gain: float32 [768], replicated, may hold values from 0.1 to 1.9
- second_shift: float32 [768], replicated, may hold values from -3 to 3
- vision_up: bfloat16 [768, 3072], replicated, may hold values from -0.21875 to 0.21875
- vision_up_bias: float32 [3072], replicated, may hold values from -3 to 3
- vision_down: bfloat16 [3072, 768], replicated, may hold values from -0.109375 to 0.109375
- vision_down_bias: float32 [768], replicated, may hold values from -3 to 3
- language_up: bfloat16 [768, 3072], replicated, may hold values from -0.21875 to 0.21875
- language_up_bias: float32 [3072], replicated, may hold values from -3 to 3
- language_down: bfloat16 [3072, 768], replicated, may hold values from -0.109375 to 0.109375
- language_down_bias: float32 [768], replicated, may hold values from -3 to 3
- image_cotangent: bfloat16 [48, 576, 768], P('pairs', 'stream'), may hold values from -6 to 6
- caption_cotangent: bfloat16 [48, 40, 768], P('pairs', 'stream'), may hold values from -6 to 6
Outputs:
- image_out: bfloat16 [48, 576, 768], P('pairs', 'stream')
- caption_out: bfloat16 [48, 40, 768], P('pairs', 'stream')
- image_grad: float32 [48, 576, 768], P('pairs', 'stream')
- caption_grad: float32 [48, 40, 768], P('pairs', 'stream')
- grad_first_gain: float32 [768], replicated
- grad_first_shift: float32 [768], replicated
- grad_query_key_value: float32 [768, 2304], replicated
- grad_query_bias: float32 [768], replicated
- grad_value_bias: float32 [768], replicated
- grad_output_weight: float32 [768, 768], replicated
- grad_output_bias: float32 [768], replicated
- grad_second_gain: float32 [768], replicated
- grad_second_shift: float32 [768], replicated
- grad_vision_up: float32 [768, 3072], P(None, ('pairs', 'stream'))
- grad_vision_up_bias: float32 [3072], replicated
- grad_vision_down: float32 [3072, 768], P(('pairs', 'stream'))
- grad_vision_down_bias: float32 [768], replicated
- grad_language_up: float32 [768, 3072], P(None, ('pairs', 'stream'))
- grad_language_up_bias: float32 [3072], replicated
- grad_language_down: float32 [3072, 768], P(('pairs', 'stream'))
- grad_language_down_bias: float32 [768], replicated
The draws below stay inside these ranges and needn't reach their ends.
Inputs may be any that keep to these rules, and one draw needn't show every extreme that they name: Caption slots 0 to lengths - 1 of a pair hold its caption; the other slots are padding that no query attends to.
All inputs are finite; a program needn't handle non-finite values.
Results may differ from the reference program's by a relative error of at most 0.013.
The reference program's roundings to bfloat16 on the way count: a program that leaves them out, or rounds other values in their place, can miss the bound.
Values may be sent and summed in bfloat16 or wider, within the bound.
No kernel may reach another device: no remote copies, remote signals or barrier semaphores. Data moves between devices by JAX's collectives and lax.ppermute only.
A program may use at most 320 MiB of HBM per device.

```python
import jax
import jax.numpy as jnp
from jax import lax

D = 768
HEADS = 12
HEAD = 64
FF = 3072
IMG = 576
TXT = 40
PP = 6
PAIRS = 48


def place_ends(result, stream_key, least, top_value):
    dims = result.shape
    place = [jax.random.randint(jax.random.fold_in(stream_key, axis), (), 0, dims[axis]) for axis in range(len(dims))]
    result = result.at[tuple(place)].set(least)
    longest = dims.index(max(dims))
    place[longest] = (place[longest] + 1) % dims[longest]
    return result.at[tuple(place)].set(top_value)


def shard_levels(rng, shape, cuts, low, top_value):
    level, own = 1.0, jax.random.fold_in(rng, 6)
    for axis_at, parts in cuts:
        draws = jnp.exp(jax.random.uniform(jax.random.fold_in(own, axis_at), (parts,), jnp.float32, low / len(cuts), top_value / len(cuts)))
        level = level * jnp.repeat(draws, shape[axis_at] // parts).reshape([-1 if axis == axis_at else 1 for axis in range(len(shape))])
    return level


def normal_values(stream_key, shape, scale, most, shards=(), held_as=jnp.bfloat16):
    loudness = shard_levels(stream_key, shape, shards, -0.22, 0.18) if shards else 1.0
    values = jax.random.normal(stream_key, shape, jnp.float32) * scale * loudness
    return jnp.minimum(jnp.maximum(values, -most), most).astype(held_as)


def setup_inputs(seed: int = 0) -> dict:
    key_of = jax.random.split(jax.random.key(seed), 23)
    return {
        "images": normal_values(key_of[0], (PAIRS, IMG, D), 1.0, 6.0, ((0, 8), (1, 4))),
        "captions": normal_values(key_of[1], (PAIRS, TXT, D), 1.0, 6.0, ((0, 8), (1, 4))),
        "lengths": place_ends(jax.random.randint(key_of[2], (PAIRS,), TXT // 5, TXT + 1), jax.random.fold_in(key_of[2], 1), TXT // 5, TXT).astype(jnp.int32),
        "first_gain": jnp.clip(1.0 + 0.18 * jax.random.normal(key_of[3], (D,), jnp.float32), 0.1, 1.9),
        "first_shift": normal_values(key_of[4], (D,), 0.5, 3.0, (), jnp.float32),
        "query_key_value": normal_values(key_of[5], (D, 3 * D), D ** -0.5, 0.21875),
        "query_bias": normal_values(key_of[6], (D,), 0.5, 3.0, (), jnp.float32),
        "value_bias": normal_values(key_of[7], (D,), 0.5, 3.0, (), jnp.float32),
        "output_weight": normal_values(key_of[8], (D, D), (D // 32) ** -0.5, 1.25),
        "output_bias": normal_values(key_of[9], (D,), 0.5, 3.0, (), jnp.float32),
        "second_gain": jnp.clip(1.0 + 0.18 * jax.random.normal(key_of[10], (D,), jnp.float32), 0.1, 1.9),
        "second_shift": normal_values(key_of[11], (D,), 0.5, 3.0, (), jnp.float32),
        "vision_up": normal_values(key_of[12], (D, FF), D ** -0.5, 0.21875),
        "vision_up_bias": normal_values(key_of[13], (FF,), 0.5, 3.0, (), jnp.float32),
        "vision_down": normal_values(key_of[14], (FF, D), FF ** -0.5, 0.109375),
        "vision_down_bias": normal_values(key_of[15], (D,), 0.5, 3.0, (), jnp.float32),
        "language_up": normal_values(key_of[16], (D, FF), D ** -0.5, 0.21875),
        "language_up_bias": normal_values(key_of[17], (FF,), 0.5, 3.0, (), jnp.float32),
        "language_down": normal_values(key_of[18], (FF, D), FF ** -0.5, 0.109375),
        "language_down_bias": normal_values(key_of[19], (D,), 0.5, 3.0, (), jnp.float32),
        "image_cotangent": normal_values(key_of[20], (PAIRS, IMG, D), 1.0, 6.0, ((0, 8), (1, 4))),
        "caption_cotangent": normal_values(key_of[21], (PAIRS, TXT, D), 1.0, 6.0, ((0, 8), (1, 4))),
    }


@jax.custom_vjp
def low(v):
    return lax.optimization_barrier(v.astype(jnp.bfloat16)).astype(jnp.float32)

@jax.custom_vjp
def low_back(v):
    return v

def low_keep(v):
    return (low(v), None)

def low_pass(kept, grad):
    return (grad,)

def back_keep(v):
    return (v, None)

def back_low(kept, grad):
    return (low(grad),)
low.defvjp(low_keep, low_pass)
low_back.defvjp(back_keep, back_low)

def normalize(values, gain, shift):
    average = lax.optimization_barrier(jnp.mean(values, axis=-1, keepdims=True))
    centred = values - average
    spread_sq = lax.optimization_barrier(jnp.mean(centred * centred, axis=-1, keepdims=True))
    return centred * lax.rsqrt(spread_sq + 1e-06) * gain + shift

def expert(inputs, up_weight, up_bias, down_weight, down_bias):
    highest = lax.Precision.HIGHEST
    hidden = low_back(jnp.einsum('gld,df->glf', inputs, up_weight, precision=highest) + up_bias)
    activated = low(jax.nn.gelu(hidden, approximate=False))
    return low_back(jnp.einsum('glf,fd->gld', activated, down_weight, precision=highest) + down_bias)

def group_forward(params, image_block, caption_block, length_block):
    first_gain, first_shift, query_key_value, query_bias, value_bias, output_weight, output_bias, second_gain, second_shift, vision_up, vision_up_bias, vision_down, vision_down_bias, language_up, language_up_bias, language_down, language_down_bias = params
    highest = lax.Precision.HIGHEST
    sequence = jnp.concatenate([image_block, caption_block], axis=1)
    groups, length, width = sequence.shape
    first = low(normalize(sequence, first_gain, first_shift))
    projected = jnp.einsum('gld,de->gle', first, query_key_value, precision=highest)
    queries = low(low_back((projected[..., :width] + query_bias) * 0.125))
    keys_all = low(low_back(projected[..., width:2 * width]))
    values = low(low_back(projected[..., 2 * width:] + value_bias))
    queries = queries.reshape(groups, length, HEADS, HEAD)
    keys_all = keys_all.reshape(groups, length, HEADS, HEAD)
    values = values.reshape(groups, length, HEADS, HEAD)
    scores = low_back(jnp.einsum('gqhe,gkhe->ghqk', queries, keys_all, precision=highest))
    text_slot = jnp.arange(length, dtype=jnp.int32) - IMG
    key_valid = text_slot[None, :] < length_block[:, None]
    scores = jnp.where(key_valid[:, None, None, :], scores, -1e+30)
    row_top = lax.optimization_barrier(jnp.max(scores, axis=-1, keepdims=True))
    log_total = row_top + jnp.log(lax.optimization_barrier(jnp.sum(jnp.exp(scores - row_top), axis=-1, keepdims=True)))
    weights = low(jnp.exp(scores - log_total))
    mixed = jnp.einsum('ghqk,gkhe->gqhe', weights, values, precision=highest).reshape(groups, length, width)
    mixed = low(low_back(mixed))
    branch = low_back(jnp.einsum('gld,de->gle', mixed, output_weight, precision=highest) + output_bias)
    middle = sequence + branch
    second = low(normalize(middle, second_gain, second_shift))
    image_branch = expert(second[:, :IMG], vision_up, vision_up_bias, vision_down, vision_down_bias)
    caption_branch = expert(second[:, IMG:], language_up, language_up_bias, language_down, language_down_bias)
    return (middle[:, :IMG] + image_branch, middle[:, IMG:] + caption_branch)

def reference(images, captions, lengths, first_gain, first_shift, query_key_value, query_bias, value_bias, output_weight, output_bias, second_gain, second_shift, vision_up, vision_up_bias, vision_down, vision_down_bias, language_up, language_up_bias, language_down, language_down_bias, image_cotangent, caption_cotangent):
    raw_params = (first_gain, first_shift, query_key_value, query_bias, value_bias, output_weight, output_bias, second_gain, second_shift, vision_up, vision_up_bias, vision_down, vision_down_bias, language_up, language_up_bias, language_down, language_down_bias)
    params = tuple([member.astype(jnp.float32) for member in raw_params])
    image_values = images.astype(jnp.float32)
    caption_values = captions.astype(jnp.float32)

    def layer(layer_params, image_input, caption_input):
        blocks = image_input.shape[0] // PP
        stacked = (image_input.reshape(blocks, PP, IMG, -1), caption_input.reshape(blocks, PP, TXT, -1), lengths.reshape(blocks, PP))

        def one_block(block):
            return group_forward(layer_params, block[0], block[1], block[2])
        image_result, caption_result = lax.map(jax.checkpoint(one_block), stacked)
        return (image_result.reshape(image_input.shape), caption_result.reshape(caption_input.shape))
    outputs, pullback = jax.vjp(layer, params, image_values, caption_values)
    param_grads, image_grad, caption_grad = pullback((image_cotangent.astype(jnp.float32), caption_cotangent.astype(jnp.float32)))
    grad_first_gain, grad_first_shift, grad_query_key_value, grad_query_bias, grad_value_bias, grad_output_weight, grad_output_bias, grad_second_gain, grad_second_shift, grad_vision_up, grad_vision_up_bias, grad_vision_down, grad_vision_down_bias, grad_language_up, grad_language_up_bias, grad_language_down, grad_language_down_bias = param_grads
    return (outputs[0].astype(jnp.bfloat16), outputs[1].astype(jnp.bfloat16), image_grad, caption_grad, grad_first_gain, grad_first_shift, grad_query_key_value, grad_query_bias, grad_value_bias, grad_output_weight, grad_output_bias, grad_second_gain, grad_second_shift, grad_vision_up, grad_vision_up_bias, grad_vision_down, grad_vision_down_bias, grad_language_up, grad_language_up_bias, grad_language_down, grad_language_down_bias)
```

```python
import functools

import jax
import jax.numpy as jnp
from jax import lax
from jax.experimental import pallas as pl
from jax.experimental.pallas import tpu as pltpu
from jax.sharding import PartitionSpec as P

HEADS = 12
GROUP = 4
F32 = jnp.float32
BF16 = jnp.bfloat16
VMEM_LIMIT = 63 * 1024 * 1024
BOTH = ("pairs", "stream")


def params(steps):
    return pltpu.CompilerParams(
        dimension_semantics=("arbitrary",) * steps, vmem_limit_bytes=VMEM_LIMIT
    )


def whole(shape):
    return pl.BlockSpec(shape, lambda *_: (0,) * len(shape), pipeline_mode=pl.Buffered(1))


def mm(a, b):
    return jnp.dot(a, b, preferred_element_type=F32)


def mm_t(a, b):
    return lax.dot_general(a, b, (((1,), (1,)), ((), ())), preferred_element_type=F32)


def t_mm(a, b):
    return lax.dot_general(a, b, (((0,), (0,)), ((), ())), preferred_element_type=F32)


def standardize(values):
    centred = values - jnp.mean(values, axis=-1, keepdims=True)
    inverse = lax.rsqrt(jnp.mean(centred * centred, axis=-1, keepdims=True) + 1e-06)
    return centred * inverse, inverse


def norm_through(upstream, normed, inverse, gain):
    scaled = upstream * gain
    return (
        scaled
        - jnp.mean(scaled, axis=-1, keepdims=True)
        - normed * jnp.mean(scaled * normed, axis=-1, keepdims=True)
    ) * inverse


def column_sum(values):
    return jnp.sum(values, axis=0, keepdims=True)


def project_kernel(own, far, cap, vec, weight, query, key, value):
    width = own.shape[-1]
    rows = jnp.concatenate([own[0], far[0], cap[0]], axis=0).astype(F32)
    normed, _ = standardize(rows)
    first = (normed * vec[0:1] + vec[1:2]).astype(BF16)
    key[0] = mm(first, weight[:, width : 2 * width]).astype(BF16)
    value[0] = (mm(first, weight[:, 2 * width :]) + vec[3:4]).astype(BF16)
    query[0] = ((mm(first, weight[:, :width]) + vec[2:3]) * 0.125).astype(BF16)


def project(own, far, cap, vec, weight):
    pairs, part, width = own.shape
    rows = 2 * part + cap.shape[1]
    block = lambda n: pl.BlockSpec((1, n, width), lambda i: (i, 0, 0))
    shape = jax.ShapeDtypeStruct((pairs, rows, width), BF16)
    return pl.pallas_call(
        project_kernel,
        grid=(pairs,),
        in_specs=[block(part), block(part), block(cap.shape[1]), whole(vec.shape), whole(weight.shape)],
        out_specs=[block(rows)] * 3,
        out_shape=[shape] * 3,
        compiler_params=params(1),
        name="project",
        cost_estimate=pl.CostEstimate(
            flops=6 * pairs * rows * width * width, transcendentals=0, bytes_accessed=12_000_000
        ),
    )(own, far, cap, vec, weight)


def stack_heads(values, lanes):
    head = values.shape[-1] // GROUP
    zero = jnp.zeros_like(values)
    return jnp.concatenate(
        [jnp.where(lanes // head == h, values, zero) for h in range(GROUP)], axis=0
    )


def attend_kernel(
    query, key0, value0, key1, value1, bias, own, far, cap, vec, weight,
    mixed, total, mid_own, mid_far, mid_cap, sec_own, sec_far, sec_cap,
    scores, probs,
):
    step = pl.program_id(1)
    rows, span = query.shape[1], query.shape[2]
    part = own.shape[1]
    lanes = lax.broadcasted_iota(jnp.int32, (1, span), 1)
    keys = jnp.concatenate([key0[0], key1[0]], axis=0)
    values = jnp.concatenate([value0[0], value1[0]], axis=0)
    scores[...] = mm_t(stack_heads(query[0], lanes), keys)
    marks = lax.broadcasted_iota(jnp.int32, (1, total.shape[2]), 1)

    @pl.when(step == 0)
    def _():
        total[0] = jnp.zeros(total.shape[1:], F32)

    for h in range(GROUP):
        at = pl.ds(h * rows, rows)
        masked = scores[at] + bias[0]
        top = jnp.max(masked, axis=-1, keepdims=True)
        shifted = jnp.exp(masked - top)
        amount = jnp.sum(shifted, axis=-1, keepdims=True)
        probs[at] = (shifted * (1.0 / amount)).astype(BF16)
        total[0] = jnp.where(marks == step * GROUP + h, top + jnp.log(amount), total[0])
    head = span // GROUP
    result = jnp.zeros((rows, span), F32)
    for h in range(GROUP):
        result = jnp.where(lanes // head == h, mm(probs[pl.ds(h * rows, rows)], values), result)
    mixed[0, :, pl.ds(pl.multiple_of(step * span, span), span)] = result.astype(BF16)

    @pl.when(step == pl.num_programs(1) - 1)
    def _():
        branch = mm(mixed[0], weight[...]) + vec[4:5]
        for place, source, mid, second in (
            (0, own, mid_own, sec_own),
            (part, far, mid_far, sec_far),
            (2 * part, cap, mid_cap, sec_cap),
        ):
            count = source.shape[1]
            middle = source[0].astype(F32) + branch[place : place + count]
            mid[0] = middle
            normed, _ = standardize(middle)
            second[0] = (normed * vec[5:6] + vec[6:7]).astype(BF16)


def attend(query, key0, value0, key1, value1, bias, own, far, cap, vec, weight):
    pairs, rows, width = query.shape
    part, slots = own.shape[1], cap.shape[1]
    span = GROUP * (width // HEADS)
    keys = 2 * rows
    wide = pl.BlockSpec((1, rows, span), lambda i, j: (i, 0, j))
    block = lambda n, w=width: pl.BlockSpec((1, n, w), lambda i, j: (i, 0, 0))
    shape = lambda n, t: jax.ShapeDtypeStruct((pairs, n, width), t)
    return pl.pallas_call(
        attend_kernel,
        grid=(pairs, width // span),
        in_specs=[wide] * 5
        + [block(1, keys), block(part), block(part), block(slots), whole(vec.shape), whole(weight.shape)],
        out_specs=[block(rows), block(rows, 128)] + [block(part), block(part), block(slots)] * 2,
        out_shape=[
            shape(rows, BF16),
            jax.ShapeDtypeStruct((pairs, rows, 128), F32),
            shape(part, F32),
            shape(part, F32),
            shape(slots, F32),
            shape(part, BF16),
            shape(part, BF16),
            shape(slots, BF16),
        ],
        scratch_shapes=[
            pltpu.VMEM((GROUP * rows, keys), F32),
            pltpu.VMEM((GROUP * rows, keys), BF16),
        ],
        compiler_params=params(2),
        name="attend",
        cost_estimate=pl.CostEstimate(
            flops=20_000_000_000, transcendentals=pairs * HEADS * rows * keys, bytes_accessed=20_000_000
        ),
    )(query, key0, value0, key1, value1, bias, own, far, cap, vec, weight)


def expert_kernel(parts, with_weights, block_rows, gain_row, bias_row, *refs):
    refs = list(refs)
    take = lambda n: [refs.pop(0) for _ in range(n)]
    second_in, cotangent_in, middle_in = take(parts), take(parts), take(parts)
    vec, up, up_bias, down = take(4)
    out, back = take(parts), take(parts)
    (up_bias_grad,) = take(1)
    (sums,) = take(1)
    weight_grad = take(1)[0] if with_weights else None
    second, cotangent, hidden, active_grad, active, hidden_grad, branch, second_grad = take(8)
    step = pl.program_id(0)
    count = second_in[0].shape[0]
    width = second.shape[1]

    @pl.when(step == 0)
    def _():
        for i in range(parts):
            second[pl.ds(i * count, count)] = second_in[i][...]
            cotangent[pl.ds(i * count, count)] = cotangent_in[i][...]
        branch[...] = jnp.zeros_like(branch)
        second_grad[...] = jnp.zeros_like(second_grad)

    hidden[...] = mm(second[...], up[...])
    active_grad[...] = mm_t(cotangent[...], down[...])

    def pointwise(i, bias_grad):
        at = pl.ds(pl.multiple_of(i * block_rows, block_rows), block_rows)
        values = hidden[at] + up_bias[...]
        share = 0.5 * (1.0 + lax.erf(values * 0.7071067811865476))
        density = jnp.exp(values * values * -0.5) * 0.3989422804014327
        active[at] = (values * share).astype(BF16)
        grad = (active_grad[at] * (share + values * density)).astype(BF16)
        hidden_grad[at] = grad
        return bias_grad + column_sum(grad.astype(F32))

    rows = parts * count
    up_bias_grad[...] = lax.fori_loop(
        0, rows // block_rows, pointwise, jnp.zeros(up_bias_grad.shape, F32)
    )
    branch[...] += mm(active[...], down[...])
    second_grad[...] += mm_t(hidden_grad[...], up[...])
    if with_weights:
        weight_grad[:, :width] = t_mm(hidden_grad[...], second[...]).astype(BF16)
        weight_grad[:, width:] = t_mm(active[...], cotangent[...]).astype(BF16)

    @pl.when(step == pl.num_programs(0) - 1)
    def _():
        zero = jnp.zeros((1, width), F32)
        sums_now = (zero, zero, zero)
        for i in range(parts):

            def finish(j, carried, i=i):
                at = pl.ds(pl.multiple_of(j * block_rows, block_rows), block_rows)
                all_at = pl.ds(pl.multiple_of(i * count + j * block_rows, 16), block_rows)
                middle = middle_in[i][at]
                out[i][at] = (middle + branch[all_at] + vec[bias_row : bias_row + 1]).astype(BF16)
                normed, inverse = standardize(middle)
                grad = second_grad[all_at]
                cot = cotangent[all_at].astype(F32)
                back[i][at] = cot + norm_through(grad, normed, inverse, vec[gain_row : gain_row + 1])
                gain_sum, shift_sum, cot_sum = carried
                return (
                    gain_sum + column_sum(grad * normed),
                    shift_sum + column_sum(grad),
                    cot_sum + column_sum(cot),
                )

            sums_now = lax.fori_loop(0, count // block_rows, finish, sums_now)
        sums[...] = jnp.concatenate(sums_now + (jnp.zeros((5, width), F32),), axis=0)


def expert(seconds, cotangents, middles, vec, up, up_bias, down, chunk, block_rows, bias_row, with_weights):
    parts = len(seconds)
    count, width = seconds[0].shape
    units = up.shape[1]
    rows = parts * count
    full = whole((count, width))
    resident = pl.BlockSpec((count, width), lambda j: (0, 0))
    shape = lambda t: jax.ShapeDtypeStruct((count, width), t)
    out_specs = [resident] * (2 * parts) + [
        pl.BlockSpec((1, chunk), lambda j: (0, j)),
        pl.BlockSpec((8, width), lambda j: (0, 0)),
    ]
    out_shape = [shape(BF16)] * parts + [shape(F32)] * parts + [
        jax.ShapeDtypeStruct((1, units), F32),
        jax.ShapeDtypeStruct((8, width), F32),
    ]
    if with_weights:
        out_specs.append(pl.BlockSpec((chunk, 2 * width), lambda j: (j, 0)))
        out_shape.append(jax.ShapeDtypeStruct((units, 2 * width), BF16))
    result = pl.pallas_call(
        functools.partial(expert_kernel, parts, with_weights, block_rows, 5, bias_row),
        grid=(units // chunk,),
        in_specs=[full] * (3 * parts)
        + [
            whole(vec.shape),
            pl.BlockSpec((width, chunk), lambda j: (0, j)),
            pl.BlockSpec((1, chunk), lambda j: (0, j)),
            pl.BlockSpec((chunk, width), lambda j: (j, 0)),
        ],
        out_specs=out_specs,
        out_shape=out_shape,
        scratch_shapes=[
            pltpu.VMEM((rows, width), BF16),
            pltpu.VMEM((rows, width), BF16),
            pltpu.VMEM((rows, chunk), F32),
            pltpu.VMEM((rows, chunk), F32),
            pltpu.VMEM((rows, chunk), BF16),
            pltpu.VMEM((rows, chunk), BF16),
            pltpu.VMEM((rows, width), F32),
            pltpu.VMEM((rows, width), F32),
        ],
        compiler_params=params(1),
        name="expert_weights" if with_weights else "expert",
        cost_estimate=pl.CostEstimate(
            flops=(12 if with_weights else 8) * rows * width * units,
            transcendentals=2 * rows * units,
            bytes_accessed=30_000_000,
        ),
    )(*seconds, *cotangents, *middles, vec, up, up_bias, down)
    return result[:parts], result[parts : 2 * parts], *result[2 * parts :]


def share_kernel(second, cotangent, up, up_bias, down, up_grad, down_grad):
    values = mm(second[...], up[...]) + up_bias[...]
    share = 0.5 * (1.0 + lax.erf(values * 0.7071067811865476))
    density = jnp.exp(values * values * -0.5) * 0.3989422804014327
    active = (values * share).astype(BF16)
    active_grad = mm_t(cotangent[...], down[...])
    hidden_grad = (active_grad * (share + values * density)).astype(BF16)

    @pl.when(pl.program_id(0) == 0)
    def _():
        up_grad[...] = jnp.zeros_like(up_grad)
        down_grad[...] = jnp.zeros_like(down_grad)

    up_grad[...] += t_mm(second[...], hidden_grad)
    down_grad[...] += t_mm(active, cotangent[...])


def share_grads(second, cotangent, up, up_bias, down):
    rows, width = second.shape
    units = up.shape[1]
    block_rows = 1024
    tokens = pl.BlockSpec((block_rows, width), lambda i: (i, 0))
    return pl.pallas_call(
        share_kernel,
        grid=(rows // block_rows,),
        in_specs=[tokens, tokens, whole(up.shape), whole(up_bias.shape), whole(down.shape)],
        out_specs=[
            pl.BlockSpec((width, units), lambda i: (0, 0)),
            pl.BlockSpec((units, width), lambda i: (0, 0)),
        ],
        out_shape=[
            jax.ShapeDtypeStruct((width, units), F32),
            jax.ShapeDtypeStruct((units, width), F32),
        ],
        compiler_params=params(1),
        name="share_grads",
        cost_estimate=pl.CostEstimate(
            flops=8 * rows * width * max(units, 128), transcendentals=0, bytes_accessed=7_000_000
        ),
    )(second, cotangent, up, up_bias, down)


def attend_back_kernel(
    grad_own, grad_far, grad_cap, query, key0, value0, key1, value1, bias, mixed, total, weight,
    query_grad, key_grad0, value_grad0, key_grad1, value_grad1, weight_grad, bias_grad,
    mixed_grad, scores, prob_grad, probs, score_grad, weight_sum,
):
    pair, step = pl.program_id(0), pl.program_id(1)
    rows, span = query.shape[1], query.shape[2]
    lanes = lax.broadcasted_iota(jnp.int32, (1, span), 1)

    @pl.when(jnp.logical_and(pair == 0, step == 0))
    def _():
        weight_sum[...] = jnp.zeros_like(weight_sum)
        bias_grad[...] = jnp.zeros_like(bias_grad)

    @pl.when(step == 0)
    def _():
        branch = jnp.concatenate([grad_own[0], grad_far[0], grad_cap[0]], axis=0).astype(BF16)
        mixed_grad[...] = mm_t(branch, weight[...]).astype(BF16)
        weight_sum[...] += t_mm(mixed[0], branch)
        bias_grad[0:1] += column_sum(branch.astype(F32))

    keys = jnp.concatenate([key0[0], key1[0]], axis=0)
    values = jnp.concatenate([value0[0], value1[0]], axis=0)
    queries = stack_heads(query[0], lanes)
    upstream = stack_heads(
        mixed_grad[:, pl.ds(pl.multiple_of(step * span, span), span)], lanes
    )
    scores[...] = mm_t(queries, keys)
    prob_grad[...] = mm_t(upstream, values)
    marks = lax.broadcasted_iota(jnp.int32, (1, total.shape[2]), 1)
    for h in range(GROUP):
        at = pl.ds(h * rows, rows)
        log_total = jnp.sum(
            jnp.where(marks == step * GROUP + h, total[0], 0.0), axis=-1, keepdims=True
        )
        prob = jnp.exp(scores[at] + bias[0] - log_total)
        grad = prob_grad[at]
        centre = jnp.sum(grad * prob, axis=-1, keepdims=True)
        probs[at] = prob.astype(BF16)
        score_grad[at] = (prob * (grad - centre)).astype(BF16)
    head = span // GROUP
    result = jnp.zeros((rows, span), F32)
    for h in range(GROUP):
        result = jnp.where(lanes // head == h, mm(score_grad[pl.ds(h * rows, rows)], keys), result)
    query_grad[0] = (result.astype(BF16).astype(F32) * 0.125).astype(BF16)
    key_grad = t_mm(score_grad[...], queries)
    key_grad0[0] = key_grad[:rows]
    key_grad1[0] = key_grad[rows:].astype(BF16)
    value_grad = t_mm(probs[...], upstream)
    value_grad0[0] = value_grad[:rows]
    value_grad1[0] = value_grad[rows:].astype(BF16)

    @pl.when(jnp.logical_and(pair == pl.num_programs(0) - 1, step == pl.num_programs(1) - 1))
    def _():
        weight_grad[...] = weight_sum[...].astype(BF16)


def attend_back(grads, query, key0, value0, key1, value1, bias, mixed, total, weight):
    pairs, rows, width = query.shape
    part, slots = grads[0].shape[1], grads[2].shape[1]
    span = GROUP * (width // HEADS)
    keys = 2 * rows
    wide = pl.BlockSpec((1, rows, span), lambda i, j: (i, 0, j))
    block = lambda n, w=width: pl.BlockSpec((1, n, w), lambda i, j: (i, 0, 0))
    shape = lambda t: jax.ShapeDtypeStruct((pairs, rows, width), t)
    fixed = lambda s: pl.BlockSpec(s, lambda i, j: (0, 0))
    return pl.pallas_call(
        attend_back_kernel,
        grid=(pairs, width // span),
        in_specs=[block(part), block(part), block(slots)]
        + [wide] * 5
        + [block(1, keys), block(rows), block(rows, 128), whole(weight.shape)],
        out_specs=[wide] * 5 + [fixed((width, width)), fixed((8, width))],
        out_shape=[shape(BF16), shape(F32), shape(F32), shape(BF16), shape(BF16)]
        + [jax.ShapeDtypeStruct((width, width), BF16), jax.ShapeDtypeStruct((8, width), F32)],
        scratch_shapes=[
            pltpu.VMEM((rows, width), BF16),
            pltpu.VMEM((GROUP * rows, keys), F32),
            pltpu.VMEM((GROUP * rows, keys), F32),
            pltpu.VMEM((GROUP * rows, keys), BF16),
            pltpu.VMEM((GROUP * rows, keys), BF16),
            pltpu.VMEM((width, width), F32),
        ],
        compiler_params=params(2),
        name="attend_back",
        cost_estimate=pl.CostEstimate(
            flops=40_000_000_000, transcendentals=pairs * HEADS * rows * keys, bytes_accessed=40_000_000
        ),
    )(*grads, query, key0, value0, key1, value1, bias, mixed, total, weight)


def finish_kernel(
    query_grad, key_grad, value_grad, key_more, value_more, own, far, cap,
    grad_own, grad_far, grad_cap, vec, weight,
    in_own, in_far, in_cap, weight_grad, sums, weight_sum,
):
    pair = pl.program_id(0)
    width, part = own.shape[2], own.shape[1]

    @pl.when(pair == 0)
    def _():
        weight_sum[...] = jnp.zeros_like(weight_sum)
        sums[...] = jnp.zeros_like(sums)

    rows = jnp.concatenate([own[0], far[0], cap[0]], axis=0).astype(F32)
    normed, inverse = standardize(rows)
    first = (normed * vec[0:1] + vec[1:2]).astype(BF16)
    query = query_grad[0]
    key = (key_grad[0] + key_more[0].astype(F32)).astype(BF16)
    value = (value_grad[0] + value_more[0].astype(F32)).astype(BF16)
    first_grad = (
        mm_t(query, weight[:, :width])
        + mm_t(key, weight[:, width : 2 * width])
        + mm_t(value, weight[:, 2 * width :])
    )
    weight_sum[:, :width] += t_mm(first, query)
    weight_sum[:, width : 2 * width] += t_mm(first, key)
    weight_sum[:, 2 * width :] += t_mm(first, value)
    through = norm_through(first_grad, normed, inverse, vec[0:1])
    in_own[0] = grad_own[0] + through[:part]
    in_far[0] = (grad_far[0] + through[part : 2 * part]).astype(BF16)
    in_cap[0] = grad_cap[0] + through[2 * part :]
    sums[...] += jnp.concatenate(
        [
            column_sum(first_grad * normed),
            column_sum(first_grad),
            column_sum(query.astype(F32)),
            column_sum(value.astype(F32)),
            jnp.zeros((4, width), F32),
        ],
        axis=0,
    )

    @pl.when(pair == pl.num_programs(0) - 1)
    def _():
        weight_grad[...] = weight_sum[...].astype(BF16)


def finish(query_grad, key_grad, value_grad, key_more, value_more, own, far, cap, grads, vec, weight):
    pairs, rows, width = query_grad.shape
    part, slots = own.shape[1], cap.shape[1]
    block = lambda n: pl.BlockSpec((1, n, width), lambda i: (i, 0, 0))
    fixed = lambda s: pl.BlockSpec(s, lambda i: (0, 0))
    shape = lambda n, t: jax.ShapeDtypeStruct((pairs, n, width), t)
    split = [block(part), block(part), block(slots)]
    return pl.pallas_call(
        finish_kernel,
        grid=(pairs,),
        in_specs=[block(rows)] * 5 + split + split + [whole(vec.shape), whole(weight.shape)],
        out_specs=split + [fixed((width, 3 * width)), fixed((8, width))],
        out_shape=[shape(part, F32), shape(part, BF16), shape(slots, F32)]
        + [jax.ShapeDtypeStruct((width, 3 * width), BF16), jax.ShapeDtypeStruct((8, width), F32)],
        scratch_shapes=[pltpu.VMEM((width, 3 * width), F32)],
        compiler_params=params(1),
        name="finish",
        cost_estimate=pl.CostEstimate(
            flops=12 * pairs * rows * width * width, transcendentals=0, bytes_accessed=30_000_000
        ),
    )(query_grad, key_grad, value_grad, key_more, value_more, own, far, cap, *grads, vec, weight)


def local(
    images,
    captions,
    lengths,
    first_gain,
    first_shift,
    query_key_value,
    query_bias,
    value_bias,
    output_weight,
    output_bias,
    second_gain,
    second_shift,
    vision_up,
    vision_up_bias,
    vision_down,
    vision_down_bias,
    language_up,
    language_up_bias,
    language_down,
    language_down_bias,
    image_cotangent,
    caption_cotangent,
):
    pair_count, part, width = images.shape
    slots = captions.shape[1]
    streams = lax.axis_size("stream")
    stream = lax.axis_index("stream")
    side, core = stream // 2, stream % 2
    half = pair_count // 2
    across = [(i, (i + 2) % streams) for i in range(streams)]
    beside = [(i, i ^ 1) for i in range(streams)]

    def keep(values):
        return lax.dynamic_slice_in_dim(values, side * half, half, 0)

    def swap(values):
        return lax.ppermute(
            lax.dynamic_slice_in_dim(values, (1 - side) * half, half, 0), "stream", across
        )

    caption_rows = -(-2 * slots // 32) * 32

    def caption_block(mine, theirs):
        filler = jnp.zeros((half, caption_rows - 2 * slots, width), mine.dtype)
        return jnp.concatenate([mine, theirs, filler], axis=1)

    own, far = keep(images), swap(images)
    cap = caption_block(keep(captions), swap(captions))
    vec = jnp.stack(
        [
            first_gain,
            first_shift,
            query_bias,
            value_bias,
            output_bias,
            second_gain,
            second_shift,
            vision_down_bias,
            language_down_bias,
        ]
    )
    rows = 2 * part + caption_rows
    place = jnp.arange(2 * rows, dtype=jnp.int32)
    within = place % rows
    slot = within - 2 * part
    from_core = jnp.where(place < rows, core, 1 - core)
    from_side = jnp.where(slot < slots, side, 1 - side)
    index = (2 * from_side + from_core) * slots + slot % slots
    limit = jnp.where(slot < 2 * slots, index, jnp.int32(2**30))
    limit = jnp.where(within < 2 * part, -1, limit)
    bias = jnp.where(limit[None, :] < keep(lengths)[:, None], 0.0, -1e30)[:, None, :]

    query, key0, value0 = project(own, far, cap, vec, query_key_value)
    key1 = lax.ppermute(key0, "stream", beside)
    value1 = lax.ppermute(value0, "stream", beside)
    cot_own, cot_far = keep(image_cotangent), swap(image_cotangent)
    cot_cap = caption_block(keep(caption_cotangent), swap(caption_cotangent))

    mixed, total, mid_own, mid_far, mid_cap, sec_own, sec_far, sec_cap = attend(
        query, key0, value0, key1, value1, bias, own, far, cap, vec, output_weight
    )
    flat = lambda values: values.reshape(-1, width)
    (out_own, out_far), (grad_own, grad_far), vision_up_bias_grad, vision_sums, vision_grad = expert(
        [flat(sec_own), flat(sec_far)],
        [flat(cot_own), flat(cot_far)],
        [flat(mid_own), flat(mid_far)],
        vec,
        vision_up,
        vision_up_bias[None],
        vision_down,
        512,
        48,
        7,
        True,
    )
    (out_cap,), (grad_cap,), language_up_bias_grad, language_sums = expert(
        [flat(sec_cap)],
        [flat(cot_cap)],
        [flat(mid_cap)],
        vec,
        language_up,
        language_up_bias[None],
        language_down,
        512,
        48,
        8,
        False,
    )
    devices = lax.axis_size("pairs") * streams
    position = lax.axis_index("pairs") * streams + stream

    def gather_captions(values):
        tokens = values[:, : 2 * slots].reshape(-1, width)
        extra = -tokens.shape[0] % 64
        tokens = jnp.concatenate([tokens, jnp.zeros((extra, width), tokens.dtype)], axis=0)
        return lax.all_gather(tokens, BOTH, axis=0, tiled=True)

    units = language_up.shape[1] // devices
    language_up_grad, language_down_grad = share_grads(
        gather_captions(sec_cap),
        gather_captions(cot_cap),
        lax.dynamic_slice_in_dim(language_up, position * units, units, 1),
        lax.dynamic_slice_in_dim(language_up_bias, position * units, units, 0)[None],
        lax.dynamic_slice_in_dim(language_down, position * units, units, 0),
    )
    vision_share = lax.psum_scatter(vision_grad, BOTH, scatter_dimension=0, tiled=True).astype(F32)
    vision_up_grad = vision_share[:, :width].T
    vision_down_grad = vision_share[:, width:]

    grads = [v.reshape(half, -1, width) for v in (grad_own, grad_far, grad_cap)]
    query_grad, key_grad0, value_grad0, key_grad1, value_grad1, output_grad, output_sums = attend_back(
        grads, query, key0, value0, key1, value1, bias, mixed, total, output_weight
    )
    key_more = lax.ppermute(key_grad1, "stream", beside)
    value_more = lax.ppermute(value_grad1, "stream", beside)
    in_own, in_far, in_cap, projection_grad, first_sums = finish(
        query_grad, key_grad0, value_grad0, key_more, value_more, own, far, cap, grads, vec, query_key_value
    )
    projection_grad = lax.psum(projection_grad, BOTH).astype(F32)
    output_grad = lax.psum(output_grad, BOTH).astype(F32)
    small = jnp.concatenate(
        [
            first_sums[:4],
            output_sums[:1],
            vision_sums[:3],
            language_sums[:3],
            vision_up_bias_grad.reshape(-1, width),
            language_up_bias_grad.reshape(-1, width),
        ],
        axis=0,
    )
    small = lax.psum(small, BOTH)
    wide = vision_up_bias.shape[0] // width

    def home(mine, theirs, kind):
        theirs = lax.ppermute(theirs, "stream", across).astype(kind)
        base = jnp.zeros((pair_count,) + mine.shape[1:], kind)
        base = lax.dynamic_update_slice_in_dim(base, mine.astype(kind), side * half, 0)
        return lax.dynamic_update_slice_in_dim(base, theirs, (1 - side) * half, 0)

    shaped = lambda values: values.reshape(half, -1, width)
    out_cap = shaped(out_cap)
    return (
        home(shaped(out_own), shaped(out_far), BF16),
        home(out_cap[:, :slots], out_cap[:, slots : 2 * slots], BF16),
        home(in_own, in_far, F32),
        home(in_cap[:, :slots], in_cap[:, slots : 2 * slots], F32),
        small[0],
        small[1],
        projection_grad,
        small[2],
        small[3],
        output_grad,
        small[4],
        small[5] + small[8],
        small[6] + small[9],
        vision_up_grad,
        small[11 : 11 + wide].reshape(-1),
        vision_down_grad,
        small[7],
        language_up_grad,
        small[11 + wide : 11 + 2 * wide].reshape(-1),
        language_down_grad,
        small[10],
    )


def solution(mesh):
    rows = P("pairs", "stream", None)
    return jax.shard_map(
        local,
        mesh=mesh,
        in_specs=(rows, rows, P("pairs")) + (P(),) * 17 + (rows, rows),
        out_specs=(rows,) * 4
        + (P(),) * 9
        + (
            P(None, BOTH),
            P(),
            P(BOTH, None),
            P(),
            P(None, BOTH),
            P(),
            P(BOTH, None),
            P(),
        ),
        check_vma=False,
    )
```
